32 devices in a mesh: section: 4 (over z), dp: 8 (over y, x, core).
Axes of the slice: x: 2, y: 2, z: 4, core: 2. Of those that a mesh axis runs over, the one named last changes fastest.
Arguments:
- inject: bfloat16 [4, 64, 4096], P('section', 'dp'), may hold values from -42 to 42, as said below
- w_gate: bfloat16 [4, 4096, 11008], P('section', None, 'dp'), may hold values from -0.09375 to 0.09375
- w_up: bfloat16 [4, 4096, 11008], P('section', None, 'dp'), may hold values from -0.09375 to 0.09375
- w_down: bfloat16 [4, 11008, 4096], P('section', 'dp'), may hold values from -0.0546875 to 0.0546875
- gain: float32 [4, 4096], P('section'), may hold values from 0.5 to 1.5
Outputs:
- iterate: float32 [4, 64, 4096], P('section', 'dp')
- mixing: float32 [4, 5, 5], P('section')
The draws below stay inside these ranges and needn't reach their ends.
Inputs may be any that keep to these rules, and one draw needn't show every extreme that they name: inject has entries of varied magnitude from token to token.
All inputs are finite; a program needn't handle non-finite values.
Results may differ from the reference program's by a relative error of at most 0.0038.
Values may be sent and summed in bfloat16 or wider, within the bound.
A program may use at most 128 MiB of HBM per device.

```python
import math
import jax
import jax.numpy as jnp
from jax import lax

D = 4096
FF = 11008
ITERS = 5
HIST = 5
SECTIONS = 4
TOKENS = 64
N_DP = 8


def draw_inject(key, part):
    first = jax.random.fold_in(key, 11)
    second = jax.random.fold_in(key, 12)
    ramp = 3.0 ** (jnp.arange(TOKENS, dtype=jnp.float32) / TOKENS)
    base = jnp.clip(jax.random.normal(first, (SECTIONS, TOKENS, D), jnp.float32), -4.0, 4.0)
    scales = jnp.exp(jax.random.uniform(second, (SECTIONS, TOKENS, 1), jnp.float32, math.log(0.3), math.log(3.0)))
    values = jnp.clip(base * ramp[None, :, None] * scales, -42.0, 42.0)
    values = values.at[0, TOKENS - 1, 0].set(42.0).at[0, TOKENS - 1, 1].set(-42.0)
    return values.astype(jnp.bfloat16)


def block_levels(rng, dims, pieces, low, largest):
    def one(dim, parts):
        steps = jax.random.uniform(jax.random.fold_in(jax.random.fold_in(rng, 6), dim), (parts,), jnp.float32, low / len(pieces), largest / len(pieces))
        return jnp.repeat(jnp.exp(steps), dims[dim] // parts).reshape((-1,) + (1,) * (len(dims) - dim - 1))

    factor_of = one(*pieces[0])
    for cut in pieces[1:]:
        factor_of = factor_of * one(*cut)
    return factor_of


def bell_draw(rng, shape, spread, limit, shards=(), kind=jnp.bfloat16):
    factor_of = block_levels(rng, shape, shards, -0.22, 0.18) if shards else 1.0
    values = jax.random.normal(rng, shape, jnp.float32) * spread * factor_of
    return jnp.minimum(jnp.maximum(values, -limit), limit).astype(kind)


def setup_inputs(seed: int = 0) -> dict:
    splits = jax.random.split(jax.random.key(seed), 6)
    return {
        "inject": draw_inject(jax.random.fold_in(splits[5], 71), 0),
        "w_gate": bell_draw(splits[1], (SECTIONS, D, FF), D ** -0.5, 0.09375, ((0, 4), (2, 8))),
        "w_up": bell_draw(splits[2], (SECTIONS, D, FF), D ** -0.5, 0.09375, ((0, 4), (2, 8))),
        "w_down": bell_draw(splits[3], (SECTIONS, FF, D), FF ** -0.5, 0.0546875, ((0, 4), (1, 8))),
        "gain": jnp.clip(1.0 + 0.1 * jax.random.normal(splits[4], (SECTIONS, D), jnp.float32), 0.5, 1.5),
    }


def rms_scaled(values, gain_row):
    inverse = lax.rsqrt(lax.optimization_barrier(jnp.mean(values * values, axis=-1, keepdims=True)) + 1e-06)
    return (values * inverse * gain_row).astype(jnp.bfloat16)

def solve_small(system, target):
    count = system.shape[-1]
    entries = [[system[..., i, j] for j in range(count)] for i in range(count)]
    values = [target[..., i] for i in range(count)]
    for p in range(count):
        for i in range(p + 1, count):
            factor = entries[i][p] / entries[p][p]
            for j in range(p, count):
                entries[i][j] = entries[i][j] - factor * entries[p][j]
            values[i] = values[i] - factor * values[p]
    answer = [None] * count
    for i in range(count - 1, -1, -1):
        accum = values[i]
        for j in range(i + 1, count):
            accum = accum - entries[i][j] * answer[j]
        answer[i] = accum / entries[i][i]
    return jnp.stack(answer, axis=-1)

def mixing_weights(matrix, iteration):
    live = (jnp.arange(HIST) <= iteration).astype(jnp.float32)
    damp = 0.01 * jnp.trace(matrix, axis1=-2, axis2=-1) / (iteration + 1) + 1e-06
    eye_mat = jnp.eye(HIST, dtype=jnp.float32)
    diagonal = live * damp[..., None] + (1.0 - live)
    system = matrix * live[:, None] * live[None, :] + eye_mat * diagonal[..., None, :]
    target = jnp.broadcast_to(live, system.shape[:-1])
    beta = solve_small(system, target)
    return beta / lax.optimization_barrier(jnp.sum(beta, axis=-1, keepdims=True))

def block_out(operands):
    values, gate_w, up_w, down_w, gain_row = operands
    normed = rms_scaled(values, gain_row)
    gate_val = jnp.dot(normed, gate_w, preferred_element_type=jnp.float32)
    up_val = jnp.dot(normed, up_w, preferred_element_type=jnp.float32)
    hidden = (jax.nn.silu(gate_val) * up_val).astype(jnp.bfloat16)
    grouped = hidden.reshape(TOKENS, N_DP, FF // N_DP).transpose(1, 0, 2).astype(jnp.float32)
    down_groups = down_w.reshape(N_DP, FF // N_DP, D).astype(jnp.float32)
    partials = jnp.einsum('gtf,gfd->gtd', grouped, down_groups).astype(jnp.bfloat16).astype(jnp.float32)
    total = lax.optimization_barrier(jnp.sum(partials, axis=0))
    return (values + total).astype(jnp.bfloat16)

def reference(inject, w_gate, w_up, w_down, gain):
    source = inject.astype(jnp.float32)
    iterate = jnp.zeros((SECTIONS, TOKENS, D), jnp.float32)
    images = jnp.zeros((HIST, SECTIONS, TOKENS, D), jnp.float32)
    misfits = jnp.zeros((HIST, SECTIONS, TOKENS, D), jnp.float32)
    mixing = jnp.zeros((SECTIONS, ITERS, HIST), jnp.float32)
    cell_count = float(TOKENS * D)
    for iteration in range(ITERS):
        output = lax.map(block_out, (iterate, w_gate, w_up, w_down, gain))
        mapped = source + 0.5 * jnp.roll(output, 1, axis=0).astype(jnp.float32)
        misfit = mapped - iterate
        images = images.at[iteration].set(mapped)
        misfits = misfits.at[iteration].set(misfit)
        gram_matrix = jnp.einsum('hstd,gstd->shg', misfits, misfits, precision=lax.Precision.HIGHEST) / cell_count
        weights = mixing_weights(gram_matrix, iteration)
        mixing = mixing.at[:, iteration].set(weights)
        iterate = jnp.einsum('sh,hstd->std', weights, images, precision=lax.Precision.HIGHEST)
    return (iterate, mixing)
```

```python
import functools

import jax
import jax.numpy as jnp
from jax import lax
from jax.experimental import pallas as pl
from jax.experimental.pallas import tpu as pltpu
from jax.sharding import PartitionSpec as P

ITERS = 5
HIST = 5
MESH = pl.DeviceIdType.MESH
F32 = jnp.float32
BF16 = jnp.bfloat16
ROW_CUTS = 4


def solve_small(entries, values):
    count = len(values)
    for p in range(count):
        for i in range(p + 1, count):
            factor = entries[i][p] / entries[p][p]
            for j in range(p, count):
                entries[i][j] = entries[i][j] - factor * entries[p][j]
            values[i] = values[i] - factor * values[p]
    answer = [None] * count
    for i in range(count - 1, -1, -1):
        accum = values[i]
        for j in range(i + 1, count):
            accum = accum - entries[i][j] * answer[j]
        answer[i] = accum / entries[i][i]
    return answer


def kernel(
    n_sec, n_dp,
    inj_ref, gate_hbm, up_hbm, down_hbm, gain_ref,
    out_ref, mix_ref,
    w_gate, w_up, w_down,
    inj_all, inj, x, xg, inv, hidden,
    outs, misfits, acc, gram,
    pair_send, pair_recv, pair_mine, rs_send, rs_recv, out_send, mix_s,
    w_sem, inj_ssem, inj_rsem, pair_ssem, pair_rsem, rs_ssem, rs_rsem,
    z_ssem, ag_ssem, ag_rsem,
):
    sec = lax.axis_index("section")
    me = lax.axis_index("dp")
    chips = n_dp // 2
    chip = me // 2
    core = me % 2
    other = chip * 2 + 1 - core
    rows, feats = inj_ref.shape
    tokens = inj.shape[0]
    block = feats // n_dp
    hid = hidden.shape[1]
    after = (sec + 1) % n_sec
    before = (sec + n_sec - 1) % n_sec

    def cols(b):
        return pl.ds(pl.multiple_of(b * block, block), block)

    def remote(src, dst, ssem, rsem, device):
        return pltpu.make_async_remote_copy(
            src_ref=src, dst_ref=dst, send_sem=ssem, recv_sem=rsem,
            device_id=device, device_id_type=MESH,
        )

    def weight_copies(which):
        copies = []
        for a in which:
            src, dst = ((gate_hbm, w_gate), (up_hbm, w_up), (down_hbm, w_down))[a]
            size = dst.shape[0]
            edges = [size * c // ROW_CUTS // 32 * 32 for c in range(ROW_CUTS)] + [size]
            for c in range(ROW_CUTS):
                part = pl.ds(edges[c], edges[c + 1] - edges[c])
                copies.append(
                    pltpu.make_async_copy(src.at[0, part], dst.at[part], w_sem.at[a, c])
                )
        return copies

    for copy in weight_copies((0, 1, 2)):
        copy.start()

    barrier = pltpu.get_barrier_semaphore()
    for off in range(1, n_dp):
        pl.semaphore_signal(barrier, inc=1, device_id=(sec, (me + off) % n_dp), device_id_type=MESH)
    pl.semaphore_signal(barrier, inc=1, device_id=(after, me), device_id_type=MESH)
    pl.semaphore_signal(barrier, inc=1, device_id=(before, me), device_id_type=MESH)
    pl.semaphore_wait(barrier, n_dp + 1)

    def inject_copy(off):
        return remote(
            inj_ref, inj_all.at[me], inj_ssem.at[off], inj_rsem.at[me],
            (sec, (me + off) % n_dp),
        )

    for off in range(1, n_dp):
        inject_copy(off).start()

    gram[...] = jnp.zeros_like(gram)
    acc[...] = jnp.zeros_like(acc)

    inj[pl.ds(pl.multiple_of(me * rows, rows), rows), :] = inj_ref[...].astype(F32)
    for off in range(1, n_dp):
        peer = (me + n_dp - off) % n_dp
        remote(
            inj_ref, inj_all.at[peer], inj_ssem.at[off], inj_rsem.at[peer], (sec, peer)
        ).wait_recv()
        inj[pl.ds(pl.multiple_of(peer * rows, rows), rows), :] = inj_all[peer].astype(F32)

    def fold(values):
        return jnp.sum(values.reshape(tokens // 8, 8, block), axis=0)

    def add_gram(k, b):
        def one(j, carry):
            acc[j] = acc[j] + fold(misfits[k, :, cols(b)] * misfits[j, :, cols(b)])
            return carry

        lax.fori_loop(0, k + 1, one, 0)

    def finish(k):
        for j in range(HIST):
            total = jnp.sum(jnp.sum(acc[j], axis=0, keepdims=True), axis=1, keepdims=True)
            value = jnp.broadcast_to(total / float(tokens * feats), (8, 128))
            gram[k, j] = value
            gram[j, k] = value
        acc[...] = jnp.zeros_like(acc)
        live = [jnp.where(i <= k, 1.0, 0.0).astype(F32) for i in range(HIST)]
        trace = gram[0, 0]
        for i in range(1, HIST):
            trace = trace + gram[i, i]
        damp = 0.01 * trace / jnp.full((8, 128), k + 1, jnp.int32).astype(F32) + 1e-06
        system = [
            [
                gram[i, j] * (live[i] * live[j])
                + ((live[i] * damp + (1.0 - live[i])) if i == j else 0.0)
                for j in range(HIST)
            ]
            for i in range(HIST)
        ]
        beta = solve_small(system, [jnp.full((8, 128), live[i], F32) for i in range(HIST)])
        whole = beta[0]
        for i in range(1, HIST):
            whole = whole + beta[i]
        scale = jnp.float32(0.0)
        for i in range(HIST):
            weight = (beta[i] / whole)[0, 0]
            mix_ref[k, i] = weight
            mix_s[i] = weight
            scale = scale + weight

        def one(b, square):
            def slot(i, value):
                return value + (0.5 * mix_s[i]) * outs[i - 1, b].astype(F32)

            value = lax.fori_loop(1, k + 1, slot, scale * inj[:, cols(b)])
            x[:, cols(b)] = value
            xg[:, cols(b)] = (value * gain_ref[:, cols(b)]).astype(BF16)
            squared = value * value
            for g in range(block // 128):
                square = square + squared[:, g * 128 : (g + 1) * 128]
            return square

        square = lax.fori_loop(0, n_dp, one, jnp.zeros((tokens, 128), F32))
        mean = jnp.sum(square, axis=1, keepdims=True) / float(feats)
        inv[...] = jnp.broadcast_to(lax.rsqrt(mean + 1e-06), (tokens, 128))

    def first(b, carry):
        misfits[0, :, cols(b)] = inj[:, cols(b)]
        add_gram(0, b)
        return carry

    lax.fori_loop(0, n_dp, first, 0)
    finish(0)

    for off in range(1, n_dp):
        inject_copy(off).wait_send()

    def iteration(k, carry):
        q = k - 1

        @pl.when(k == 1)
        def _():
            for copy in weight_copies((0, 1)):
                copy.wait()

        start = 0
        while start < hid:
            width = min(256, hid - start)
            tile = pl.ds(start, width)
            gate_val = jnp.dot(xg[...], w_gate[:, tile], preferred_element_type=F32)
            up_val = jnp.dot(xg[...], w_up[:, tile], preferred_element_type=F32)
            factor = inv[:, :1]
            gate_val = gate_val * factor
            up_val = up_val * factor
            hidden[:, tile] = (gate_val / (1.0 + jnp.exp(-gate_val)) * up_val).astype(BF16)
            start += width

        @pl.when(k == 1)
        def _():
            for copy in weight_copies((2,)):
                copy.wait()

        def pair_copy(t):
            return remote(
                pair_send.at[t], pair_recv.at[q, t], pair_ssem.at[t], pair_rsem.at[q, t],
                (sec, other),
            )

        def rs_copy(t):
            target = ((chip + 1 + t) % chips) * 2 + core
            return remote(
                rs_send.at[t], rs_recv.at[q, t], rs_ssem.at[t], rs_rsem.at[q, t],
                (sec, target),
            )

        def pass_on(t):
            pair_copy(t).wait_recv()
            rs_send[t] = (pair_mine[t] + pair_recv[q, t].astype(F32)).astype(BF16)
            rs_copy(t).start()

        def down(t, carry):
            aim = (chip + 1 + t) % chips
            theirs = jnp.dot(
                hidden[...], w_down[:, cols(2 * aim + 1 - core)], preferred_element_type=F32
            )
            pair_send[t] = theirs.astype(BF16)
            pair_copy(t).start()
            pair_mine[t] = jnp.dot(
                hidden[...], w_down[:, cols(2 * aim + core)], preferred_element_type=F32
            )

            @pl.when(t >= 1)
            def _():
                pass_on(t - 1)

            return carry

        lax.fori_loop(0, chips, down, 0)

        pair_copy(chips - 1).wait_recv()
        total = pair_mine[chips - 1] + pair_recv[q, chips - 1].astype(F32)

        def collect(t, value):
            rs_copy(t).wait_recv()
            return value + rs_recv[q, t].astype(F32)

        total = lax.fori_loop(0, chips - 1, collect, total)
        out_send[...] = (x[:, cols(me)] + total).astype(BF16)

        def ag_copy(b, slot, device):
            return remote(
                outs.at[q, b], outs.at[q, b], ag_ssem.at[slot], ag_rsem.at[q, b], device
            )

        z_copy = remote(out_send, outs.at[q, me], z_ssem, ag_rsem.at[q, me], (after, me))
        z_copy.start()

        def absorb(b):
            value = inj[:, cols(b)] + 0.5 * outs[q, b].astype(F32) - x[:, cols(b)]
            misfits[k, :, cols(b)] = value
            add_gram(k, b)

        z_copy.wait_recv()

        def spread(t, carry):
            ag_copy(me, t, (sec, ((chip + 1 + t) % chips) * 2 + core)).start()
            return carry

        lax.fori_loop(0, chips - 1, spread, 0)
        ag_copy(me, chips - 1, (sec, other)).start()
        absorb(me)

        def forward(t, carry):
            b = ((chip + chips - 1 - t) % chips) * 2 + core
            ag_copy(b, chips + t, (sec, other)).wait_recv()
            ag_copy(b, chips + t, (sec, other)).start()
            absorb(b)
            return carry

        lax.fori_loop(0, chips - 1, forward, 0)

        def last(t, carry):
            b = ((chip + chips - t) % chips) * 2 + 1 - core
            ag_copy(b, 0, (sec, other)).wait_recv()
            absorb(b)
            return carry

        lax.fori_loop(0, chips, last, 0)
        finish(k)

        def drain(t, carry):
            pair_copy(t).wait_send()
            return carry

        lax.fori_loop(0, chips, drain, 0)

        def drain_rs(t, carry):
            rs_copy(t).wait_send()
            return carry

        lax.fori_loop(0, chips - 1, drain_rs, 0)
        z_copy.wait_send()

        def drain_ag(t, carry):
            ag_copy(me, t, (sec, other)).wait_send()
            return carry

        lax.fori_loop(0, 2 * chips - 1, drain_ag, 0)
        return carry

    lax.fori_loop(1, ITERS, iteration, 0)
    out_ref[...] = x[pl.ds(pl.multiple_of(me * rows, rows), rows), :]


def solution(mesh):
    n_sec, n_dp = mesh.shape["section"], mesh.shape["dp"]
    chips = n_dp // 2

    def local(inject, w_gate, w_up, w_down, gain):
        rows, feats = inject.shape[1:]
        hid = w_gate.shape[2]
        tokens = rows * n_dp
        block = feats // n_dp
        rounds = ITERS - 1
        vmem = pl.BlockSpec(memory_space=pltpu.VMEM)
        hbm = pl.BlockSpec(memory_space=pl.ANY)
        dma = pltpu.SemaphoreType.DMA
        out, mixing = pl.pallas_call(
            functools.partial(kernel, n_sec, n_dp),
            out_shape=(
                jax.ShapeDtypeStruct((rows, feats), F32),
                jax.ShapeDtypeStruct((ITERS, HIST), F32),
            ),
            in_specs=[vmem, hbm, hbm, hbm, vmem],
            out_specs=(vmem, pl.BlockSpec(memory_space=pltpu.SMEM)),
            scratch_shapes=[
                pltpu.VMEM((feats, hid), BF16),
                pltpu.VMEM((feats, hid), BF16),
                pltpu.VMEM((hid, feats), BF16),
                pltpu.VMEM((n_dp, rows, feats), BF16),
                pltpu.VMEM((tokens, feats), F32),
                pltpu.VMEM((tokens, feats), F32),
                pltpu.VMEM((tokens, feats), BF16),
                pltpu.VMEM((tokens, 128), F32),
                pltpu.VMEM((tokens, hid), BF16),
                pltpu.VMEM((rounds, n_dp, tokens, block), BF16),
                pltpu.VMEM((HIST, tokens, feats), F32),
                pltpu.VMEM((HIST, 8, block), F32),
                pltpu.VMEM((HIST, HIST, 8, 128), F32),
                pltpu.VMEM((chips, tokens, block), BF16),
                pltpu.VMEM((rounds, chips, tokens, block), BF16),
                pltpu.VMEM((chips, tokens, block), F32),
                pltpu.VMEM((chips - 1, tokens, block), BF16),
                pltpu.VMEM((rounds, chips - 1, tokens, block), BF16),
                pltpu.VMEM((tokens, block), BF16),
                pltpu.SMEM((HIST,), F32),
                dma((3, ROW_CUTS)),
                dma((n_dp,)),
                dma((n_dp,)),
                dma((chips,)),
                dma((rounds, chips)),
                dma((chips,)),
                dma((rounds, chips)),
                dma,
                dma((2 * chips,)),
                dma((rounds, n_dp)),
            ],
            compiler_params=pltpu.CompilerParams(
                collective_id=0,
                has_side_effects=True,
                vmem_limit_bytes=67043328,
            ),
        )(inject[0], w_gate, w_up, w_down, gain)
        return out[None], mixing[None]

    placed = (
        P("section", "dp", None),
        P("section", None, "dp"),
        P("section", None, "dp"),
        P("section", "dp", None),
        P("section", None),
    )
    return jax.shard_map(
        local,
        mesh=mesh,
        in_specs=placed,
        out_specs=(P("section", "dp", None), P("section", None, None)),
        check_vma=False,
    )
```

```python
import functools

import jax
import jax.numpy as jnp
from jax import lax
from jax.experimental import pallas as pl
from jax.experimental.pallas import tpu as pltpu
from jax.sharding import PartitionSpec as P

ITERS = 5
HIST = 5
MESH = pl.DeviceIdType.MESH
F32 = jnp.float32
BF16 = jnp.bfloat16


def solve_small(entries, values):
    count = len(values)
    for p in range(count):
        for i in range(p + 1, count):
            factor = entries[i][p] / entries[p][p]
            for j in range(p, count):
                entries[i][j] = entries[i][j] - factor * entries[p][j]
            values[i] = values[i] - factor * values[p]
    answer = [None] * count
    for i in range(count - 1, -1, -1):
        accum = values[i]
        for j in range(i + 1, count):
            accum = accum - entries[i][j] * answer[j]
        answer[i] = accum / entries[i][i]
    return answer


def across(left, right):
    return lax.dot_general(
        left, right, (((1,), (1,)), ((), ())), preferred_element_type=F32
    )


def kernel(
    n_sec, n_dp,
    inj_ref, gate_hbm, up_hbm, down_hbm, gain_ref,
    out_ref, mix_ref,
    w_gate, w_up, w_down,
    inj_all, inj, x, gates, ups, inv, hidden,
    outs, misfits, acc, gram,
    pair_send, pair_recv, pair_mine, rs_send, rs_recv, out_send, mix_s,
    w_sem, inj_ssem, inj_rsem, pair_ssem, pair_rsem, rs_ssem, rs_rsem,
    z_ssem, ag_ssem, ag_rsem,
):
    sec = lax.axis_index("section")
    me = lax.axis_index("dp")
    chips = n_dp // 2
    chip = me // 2
    core = me % 2
    other = chip * 2 + 1 - core
    rows, feats = inj_ref.shape
    tokens = inj.shape[0]
    parts = pair_send.shape[0] // chips
    block = feats // (n_dp * parts)
    subs = n_dp * parts
    hid = hidden.shape[1]
    after = (sec + 1) % n_sec
    before = (sec + n_sec - 1) % n_sec

    def cols(b):
        return pl.ds(pl.multiple_of(b * block, block), block)

    def remote(src, dst, ssem, rsem, device):
        return pltpu.make_async_remote_copy(
            src_ref=src, dst_ref=dst, send_sem=ssem, recv_sem=rsem,
            device_id=device, device_id_type=MESH,
        )

    def weight_copy(a, b):
        src, dst = ((gate_hbm, w_gate), (up_hbm, w_up))[a]
        return pltpu.make_async_copy(src.at[0, :, cols(b)], dst.at[:, cols(b)], w_sem.at[a, b])

    def down_copy():
        return pltpu.make_async_copy(down_hbm.at[0], w_down, w_sem.at[2, 0])

    def fetch(b, carry):
        weight_copy(0, b).start()
        weight_copy(1, b).start()
        return carry

    lax.fori_loop(0, subs, fetch, 0)
    down_copy().start()

    barrier = pltpu.get_barrier_semaphore()
    for off in range(1, n_dp):
        pl.semaphore_signal(barrier, inc=1, device_id=(sec, (me + off) % n_dp), device_id_type=MESH)
    pl.semaphore_signal(barrier, inc=1, device_id=(after, me), device_id_type=MESH)
    pl.semaphore_signal(barrier, inc=1, device_id=(before, me), device_id_type=MESH)
    pl.semaphore_wait(barrier, n_dp + 1)

    def inject_copy(src, b, slot, device):
        return remote(src, inj_all.at[b], inj_ssem.at[slot], inj_rsem.at[b], (sec, device))

    for t in range(chips - 1):
        inject_copy(inj_ref, me, t, ((chip + 1 + t) % chips) * 2 + core).start()
    inject_copy(inj_ref, me, chips - 1, other).start()

    gram[...] = jnp.zeros_like(gram)
    acc[...] = jnp.zeros_like(acc)

    def place(b, values):
        inj[pl.ds(pl.multiple_of(b * rows, rows), rows), :] = values.astype(F32)

    place(me, inj_ref[...])
    inject_copy(inj_ref, other, 0, other).wait_recv()
    place(other, inj_all[other])
    for t in range(chips - 1):
        b = ((chip + chips - 1 - t) % chips) * 2 + core
        onward = inject_copy(inj_all.at[b], b, chips + t, other)
        onward.wait_recv()
        onward.start()
        place(b, inj_all[b])
    for t in range(chips - 1):
        b = ((chip + chips - 1 - t) % chips) * 2 + 1 - core
        inject_copy(inj_ref, b, 0, other).wait_recv()
        place(b, inj_all[b])

    def fold(values):
        return jnp.sum(values.reshape(tokens // 8, 8, block), axis=0)

    def add_gram(k, b):
        def one(j, carry):
            acc[j] = acc[j] + fold(misfits[k, :, cols(b)] * misfits[j, :, cols(b)])
            return carry

        lax.fori_loop(0, k + 1, one, 0)

    def project(k, b, image, fresh):
        scaled = (image * gain_ref[:, cols(b)]).astype(BF16)
        for kept, weights in ((gates, w_gate), (ups, w_up)):
            part = across(scaled, weights[:, cols(b)])
            if fresh:
                kept[k] = part
            else:
                kept[k] = kept[k] + part

    def finish(k):
        for j in range(HIST):
            total = jnp.sum(jnp.sum(acc[j], axis=0, keepdims=True), axis=1, keepdims=True)
            value = jnp.broadcast_to(total / float(tokens * feats), (8, 128))
            gram[k, j] = value
            gram[j, k] = value
        acc[...] = jnp.zeros_like(acc)
        live = [jnp.where(i <= k, 1.0, 0.0).astype(F32) for i in range(HIST)]
        trace = gram[0, 0]
        for i in range(1, HIST):
            trace = trace + gram[i, i]
        damp = 0.01 * trace / jnp.full((8, 128), k + 1, jnp.int32).astype(F32) + 1e-06
        system = [
            [
                gram[i, j] * (live[i] * live[j])
                + ((live[i] * damp + (1.0 - live[i])) if i == j else 0.0)
                for j in range(HIST)
            ]
            for i in range(HIST)
        ]
        beta = solve_small(system, [jnp.full((8, 128), live[i], F32) for i in range(HIST)])
        whole = beta[0]
        for i in range(1, HIST):
            whole = whole + beta[i]
        scale = jnp.float32(0.0)
        for i in range(HIST):
            weight = (beta[i] / whole)[0, 0]
            mix_ref[k, i] = weight
            mix_s[i] = weight
            scale = scale + weight

        def one(b, square):
            def slot(i, value):
                return value + (0.5 * mix_s[i]) * outs[i - 1, b].astype(F32)

            value = lax.fori_loop(1, k + 1, slot, scale * inj[:, cols(b)])
            x[:, cols(b)] = value
            squared = value * value
            for g in range(block // 128):
                square = square + squared[:, g * 128 : (g + 1) * 128]
            return square

        square = lax.fori_loop(0, subs, one, jnp.zeros((tokens, 128), F32))
        mean = jnp.sum(square, axis=1, keepdims=True) / float(feats)
        inv[...] = jnp.broadcast_to(lax.rsqrt(mean + 1e-06), (tokens, 128))

    def first(b, carry):
        misfits[0, :, cols(b)] = inj[:, cols(b)]
        add_gram(0, b)
        weight_copy(0, b).wait()
        weight_copy(1, b).wait()
        project(0, b, inj[:, cols(b)], False)
        return carry

    gates[0] = jnp.zeros_like(gates[0])
    ups[0] = jnp.zeros_like(ups[0])
    lax.fori_loop(0, subs, first, 0)
    finish(0)

    for t in range(2 * chips - 1):
        inject_copy(inj_ref, me, t, other).wait_send()

    def iteration(k, carry):
        q = k - 1

        start = 0
        while start < hid:
            width = min(256, hid - start)
            tile = pl.ds(start, width)

            def blend(i, pair):
                weight = mix_s[i]
                return pair[0] + weight * gates[i, :, tile], pair[1] + weight * ups[i, :, tile]

            empty = jnp.zeros((tokens, width), F32)
            gate_val, up_val = lax.fori_loop(0, k, blend, (empty, empty))
            factor = inv[:, :1]
            gate_val = gate_val * factor
            up_val = up_val * factor
            hidden[:, tile] = (gate_val / (1.0 + jnp.exp(-gate_val)) * up_val).astype(BF16)
            start += width

        @pl.when(k == 1)
        def _():
            down_copy().wait()

        def pair_copy(h, t):
            r = h * chips + t
            return remote(
                pair_send.at[r], pair_recv.at[q, r], pair_ssem.at[r], pair_rsem.at[q, r],
                (sec, other),
            )

        def rs_copy(h, t):
            r = h * (chips - 1) + t
            target = ((chip + 1 + t) % chips) * 2 + core
            return remote(
                rs_send.at[r], rs_recv.at[q, r], rs_ssem.at[r], rs_rsem.at[q, r],
                (sec, target),
            )

        def pass_on(h, t):
            pair_copy(h, t).wait_recv()
            r = h * chips + t
            both = pair_mine[r] + pair_recv[q, r].astype(F32)
            rs_send[h * (chips - 1) + t] = both.astype(BF16)
            rs_copy(h, t).start()

        for h in range(parts):

            def down(t, carry, h=h):
                aim = (chip + 1 + t) % chips
                r = h * chips + t
                theirs = jnp.dot(
                    hidden[...],
                    w_down[:, cols((2 * aim + 1 - core) * parts + h)],
                    preferred_element_type=F32,
                )
                pair_send[r] = theirs.astype(BF16)
                pair_copy(h, t).start()
                pair_mine[r] = jnp.dot(
                    hidden[...],
                    w_down[:, cols((2 * aim + core) * parts + h)],
                    preferred_element_type=F32,
                )

                @pl.when(t >= 1)
                def _():
                    pass_on(h, t - 1)

                return carry

            lax.fori_loop(0, chips, down, 0)

        def z_copy(h):
            u = me * parts + h
            return remote(out_send.at[h], outs.at[q, u], z_ssem.at[h], ag_rsem.at[q, u], (after, me))

        for h in range(parts):
            pair_copy(h, chips - 1).wait_recv()
            r = h * chips + chips - 1
            total = pair_mine[r] + pair_recv[q, r].astype(F32)

            def collect(t, value, h=h):
                rs_copy(h, t).wait_recv()
                return value + rs_recv[q, h * (chips - 1) + t].astype(F32)

            total = lax.fori_loop(0, chips - 1, collect, total)
            out_send[h] = (x[:, cols(me * parts + h)] + total).astype(BF16)
            z_copy(h).start()

        def ag_copy(u, slot, device):
            return remote(
                outs.at[q, u], outs.at[q, u], ag_ssem.at[slot], ag_rsem.at[q, u], device
            )

        def absorb(u, fresh=False):
            image = inj[:, cols(u)] + 0.5 * outs[q, u].astype(F32)
            misfits[k, :, cols(u)] = image - x[:, cols(u)]

            @pl.when(k < ITERS - 1)
            def _():
                project(k, u, image, fresh)

            add_gram(k, u)

        for h in range(parts):
            u = me * parts + h
            z_copy(h).wait_recv()

            def spread(t, carry, h=h, u=u):
                target = ((chip + 1 + t) % chips) * 2 + core
                ag_copy(u, h * 2 * chips + t, (sec, target)).start()
                return carry

            lax.fori_loop(0, chips - 1, spread, 0)
            ag_copy(u, h * 2 * chips + chips - 1, (sec, other)).start()
            absorb(u, h == 0)
            u = other * parts + h
            ag_copy(u, 0, (sec, other)).wait_recv()
            absorb(u)

        def forward(i, carry):
            h, t = i // (chips - 1), i % (chips - 1)
            u = (((chip + chips - 1 - t) % chips) * 2 + core) * parts + h
            onward = ag_copy(u, h * 2 * chips + chips + t, (sec, other))
            onward.wait_recv()
            onward.start()
            absorb(u)
            return carry

        lax.fori_loop(0, parts * (chips - 1), forward, 0)

        def last(i, carry):
            h, t = i // (chips - 1), i % (chips - 1)
            u = (((chip + chips - 1 - t) % chips) * 2 + 1 - core) * parts + h
            ag_copy(u, 0, (sec, other)).wait_recv()
            absorb(u)
            return carry

        lax.fori_loop(0, parts * (chips - 1), last, 0)
        finish(k)

        for h in range(parts):

            def drain(t, carry, h=h):
                pair_copy(h, t).wait_send()
                return carry

            lax.fori_loop(0, chips, drain, 0)

            def drain_rs(t, carry, h=h):
                rs_copy(h, t).wait_send()
                return carry

            lax.fori_loop(0, chips - 1, drain_rs, 0)
            z_copy(h).wait_send()

            def drain_ag(t, carry, h=h):
                ag_copy(me * parts + h, h * 2 * chips + t, (sec, other)).wait_send()
                return carry

            lax.fori_loop(0, 2 * chips - 1, drain_ag, 0)
        return carry

    lax.fori_loop(1, ITERS, iteration, 0)
    out_ref[...] = x[pl.ds(pl.multiple_of(me * rows, rows), rows), :]


def solution(mesh):
    n_sec, n_dp = mesh.shape["section"], mesh.shape["dp"]
    chips = n_dp // 2

    def local(inject, w_gate, w_up, w_down, gain):
        rows, feats = inject.shape[1:]
        hid = w_gate.shape[2]
        tokens = rows * n_dp
        parts = 1
        block = feats // (n_dp * parts)
        rounds = ITERS - 1
        vmem = pl.BlockSpec(memory_space=pltpu.VMEM)
        hbm = pl.BlockSpec(memory_space=pl.ANY)
        dma = pltpu.SemaphoreType.DMA
        out, mixing = pl.pallas_call(
            functools.partial(kernel, n_sec, n_dp),
            out_shape=(
                jax.ShapeDtypeStruct((rows, feats), F32),
                jax.ShapeDtypeStruct((ITERS, HIST), F32),
            ),
            in_specs=[vmem, hbm, hbm, hbm, vmem],
            out_specs=(vmem, pl.BlockSpec(memory_space=pltpu.SMEM)),
            scratch_shapes=[
                pltpu.VMEM((hid, feats), BF16),
                pltpu.VMEM((hid, feats), BF16),
                pltpu.VMEM((hid, feats), BF16),
                pltpu.VMEM((n_dp, rows, feats), BF16),
                pltpu.VMEM((tokens, feats), F32),
                pltpu.VMEM((tokens, feats), F32),
                pltpu.VMEM((rounds, tokens, hid), F32),
                pltpu.VMEM((rounds, tokens, hid), F32),
                pltpu.VMEM((tokens, 128), F32),
                pltpu.VMEM((tokens, hid), BF16),
                pltpu.VMEM((rounds, n_dp * parts, tokens, block), BF16),
                pltpu.VMEM((HIST, tokens, feats), F32),
                pltpu.VMEM((HIST, 8, block), F32),
                pltpu.VMEM((HIST, HIST, 8, 128), F32),
                pltpu.VMEM((parts * chips, tokens, block), BF16),
                pltpu.VMEM((rounds, parts * chips, tokens, block), BF16),
                pltpu.VMEM((parts * chips, tokens, block), F32),
                pltpu.VMEM((parts * (chips - 1), tokens, block), BF16),
                pltpu.VMEM((rounds, parts * (chips - 1), tokens, block), BF16),
                pltpu.VMEM((parts, tokens, block), BF16),
                pltpu.SMEM((HIST,), F32),
                dma((3, n_dp * parts)),
                dma((n_dp,)),
                dma((n_dp,)),
                dma((parts * chips,)),
                dma((rounds, parts * chips)),
                dma((parts * chips,)),
                dma((rounds, parts * chips)),
                dma((parts,)),
                dma((2 * chips * parts,)),
                dma((rounds, n_dp * parts)),
            ],
            compiler_params=pltpu.CompilerParams(
                collective_id=0,
                has_side_effects=True,
                vmem_limit_bytes=67043328,
            ),
        )(inject[0], jnp.swapaxes(w_gate, 1, 2), jnp.swapaxes(w_up, 1, 2), w_down, gain)
        return out[None], mixing[None]

    placed = (
        P("section", "dp", None),
        P("section", None, "dp"),
        P("section", None, "dp"),
        P("section", "dp", None),
        P("section", None),
    )
    return jax.shard_map(
        local,
        mesh=mesh,
        in_specs=placed,
        out_specs=(P("section", "dp", None), P("section", None, None)),
        check_vma=False,
    )
```

```python
import functools

import jax
import jax.numpy as jnp
from jax import lax
from jax.experimental import pallas as pl
from jax.experimental.pallas import tpu as pltpu
from jax.sharding import PartitionSpec as P

ITERS = 5
HIST = 5
MESH = pl.DeviceIdType.MESH
F32 = jnp.float32
BF16 = jnp.bfloat16


def solve_small(entries, values):
    count = len(values)
    for p in range(count):
        for i in range(p + 1, count):
            factor = entries[i][p] / entries[p][p]
            for j in range(p, count):
                entries[i][j] = entries[i][j] - factor * entries[p][j]
            values[i] = values[i] - factor * values[p]
    answer = [None] * count
    for i in range(count - 1, -1, -1):
        accum = values[i]
        for j in range(i + 1, count):
            accum = accum - entries[i][j] * answer[j]
        answer[i] = accum / entries[i][i]
    return answer


def kernel(
    n_sec, n_dp,
    inj_ref, gate_hbm, up_hbm, down_hbm, gain_ref,
    out_ref, mix_ref,
    w_gate, w_up, w_down, stage,
    inj_all, inj, x, gates, ups, inv, hidden,
    outs, misfits, acc, gram,
    pair_send, pair_recv, pair_mine, rs_send, rs_recv, out_send, mix_s,
    w_sem, inj_ssem, inj_rsem, pair_ssem, pair_rsem, rs_ssem, rs_rsem,
    z_ssem, ag_ssem, ag_rsem,
):
    sec = lax.axis_index("section")
    me = lax.axis_index("dp")
    chips = n_dp // 2
    chip = me // 2
    core = me % 2
    other = chip * 2 + 1 - core
    rows, feats = inj_ref.shape
    tokens = inj.shape[0]
    parts = pair_send.shape[0] // chips
    block = feats // (n_dp * parts)
    subs = n_dp * parts
    depth = stage.shape[1]
    hid = hidden.shape[1]
    after = (sec + 1) % n_sec
    before = (sec + n_sec - 1) % n_sec

    def cols(b):
        return pl.ds(pl.multiple_of(b * block, block), block)

    def remote(src, dst, ssem, rsem, device):
        return pltpu.make_async_remote_copy(
            src_ref=src, dst_ref=dst, send_sem=ssem, recv_sem=rsem,
            device_id=device, device_id_type=MESH,
        )

    def weight_copy(a, b):
        src = (gate_hbm, up_hbm)[a]
        return pltpu.make_async_copy(src.at[0, :, cols(b)], stage.at[a, b % depth], w_sem.at[a, b])

    def down_copy():
        return pltpu.make_async_copy(down_hbm.at[0], w_down, w_sem.at[2, 0])

    def fetch(b, carry):
        weight_copy(0, b).start()
        weight_copy(1, b).start()
        return carry

    lax.fori_loop(0, depth, fetch, 0)
    down_copy().start()

    barrier = pltpu.get_barrier_semaphore()
    for off in range(1, n_dp):
        pl.semaphore_signal(barrier, inc=1, device_id=(sec, (me + off) % n_dp), device_id_type=MESH)
    pl.semaphore_signal(barrier, inc=1, device_id=(after, me), device_id_type=MESH)
    pl.semaphore_signal(barrier, inc=1, device_id=(before, me), device_id_type=MESH)
    pl.semaphore_wait(barrier, n_dp + 1)

    def inject_copy(src, b, slot, device):
        return remote(src, inj_all.at[b], inj_ssem.at[slot], inj_rsem.at[b], (sec, device))

    for t in range(chips - 1):
        inject_copy(inj_ref, me, t, ((chip + 1 + t) % chips) * 2 + core).start()
    inject_copy(inj_ref, me, chips - 1, other).start()

    gram[...] = jnp.zeros_like(gram)
    acc[...] = jnp.zeros_like(acc)

    def turn(b, carry):
        for a, dst in enumerate((w_gate, w_up)):
            weight_copy(a, b).wait()
            dst[cols(b), :] = stage[a, b % depth].T

        @pl.when(b + depth < subs)
        def _():
            fetch(b + depth, 0)

        return carry

    lax.fori_loop(0, subs // 2, turn, 0)

    def place(b, values):
        inj[pl.ds(pl.multiple_of(b * rows, rows), rows), :] = values.astype(F32)

    place(me, inj_ref[...])
    inject_copy(inj_ref, other, 0, other).wait_recv()
    place(other, inj_all[other])
    for t in range(chips - 1):
        b = ((chip + chips - 1 - t) % chips) * 2 + core
        onward = inject_copy(inj_all.at[b], b, chips + t, other)
        onward.wait_recv()
        onward.start()
        place(b, inj_all[b])
    lax.fori_loop(subs // 2, subs, turn, 0)
    for t in range(chips - 1):
        b = ((chip + chips - 1 - t) % chips) * 2 + 1 - core
        inject_copy(inj_ref, b, 0, other).wait_recv()
        place(b, inj_all[b])

    def fold(values):
        return jnp.sum(values.reshape(tokens // 8, 8, block), axis=0)

    def add_gram(k, b):
        def one(j, carry):
            acc[j] = acc[j] + fold(misfits[k, :, cols(b)] * misfits[j, :, cols(b)])
            return carry

        lax.fori_loop(0, k + 1, one, 0)

    def project(k, b, image, fresh):
        scaled = (image * gain_ref[:, cols(b)]).astype(BF16)
        for kept, weights in ((gates, w_gate), (ups, w_up)):
            part = jnp.dot(scaled, weights[cols(b), :], preferred_element_type=F32)
            if fresh:
                kept[k] = part
            else:
                kept[k] = kept[k] + part

    def finish(k):
        for j in range(HIST):
            total = jnp.sum(jnp.sum(acc[j], axis=0, keepdims=True), axis=1, keepdims=True)
            value = jnp.broadcast_to(total / float(tokens * feats), (8, 128))
            gram[k, j] = value
            gram[j, k] = value
        acc[...] = jnp.zeros_like(acc)
        live = [jnp.where(i <= k, 1.0, 0.0).astype(F32) for i in range(HIST)]
        trace = gram[0, 0]
        for i in range(1, HIST):
            trace = trace + gram[i, i]
        damp = 0.01 * trace / jnp.full((8, 128), k + 1, jnp.int32).astype(F32) + 1e-06
        system = [
            [
                gram[i, j] * (live[i] * live[j])
                + ((live[i] * damp + (1.0 - live[i])) if i == j else 0.0)
                for j in range(HIST)
            ]
            for i in range(HIST)
        ]
        beta = solve_small(system, [jnp.full((8, 128), live[i], F32) for i in range(HIST)])
        whole = beta[0]
        for i in range(1, HIST):
            whole = whole + beta[i]
        scale = jnp.float32(0.0)
        for i in range(HIST):
            weight = (beta[i] / whole)[0, 0]
            mix_ref[k, i] = weight
            mix_s[i] = weight
            scale = scale + weight

        def one(b, square):
            def slot(i, value):
                return value + (0.5 * mix_s[i]) * outs[i - 1, b].astype(F32)

            value = lax.fori_loop(1, k + 1, slot, scale * inj[:, cols(b)])
            x[:, cols(b)] = value
            squared = value * value
            for g in range(block // 128):
                square = square + squared[:, g * 128 : (g + 1) * 128]
            return square

        square = lax.fori_loop(0, subs, one, jnp.zeros((tokens, 128), F32))
        mean = jnp.sum(square, axis=1, keepdims=True) / float(feats)
        inv[...] = jnp.broadcast_to(lax.rsqrt(mean + 1e-06), (tokens, 128))

    def first(b, carry):
        misfits[0, :, cols(b)] = inj[:, cols(b)]
        add_gram(0, b)
        project(0, b, inj[:, cols(b)], False)
        return carry

    gates[0] = jnp.zeros_like(gates[0])
    ups[0] = jnp.zeros_like(ups[0])
    lax.fori_loop(0, subs, first, 0)
    finish(0)

    for t in range(2 * chips - 1):
        inject_copy(inj_ref, me, t, other).wait_send()

    def iteration(k, carry):
        q = k - 1

        start = 0
        while start < hid:
            width = min(256, hid - start)
            tile = pl.ds(start, width)

            def blend(i, pair):
                weight = mix_s[i]
                return pair[0] + weight * gates[i, :, tile], pair[1] + weight * ups[i, :, tile]

            empty = jnp.zeros((tokens, width), F32)
            gate_val, up_val = lax.fori_loop(0, k, blend, (empty, empty))
            factor = inv[:, :1]
            gate_val = gate_val * factor
            up_val = up_val * factor
            hidden[:, tile] = (gate_val / (1.0 + jnp.exp(-gate_val)) * up_val).astype(BF16)
            start += width

        @pl.when(k == 1)
        def _():
            down_copy().wait()

        def pair_copy(h, t):
            r = h * chips + t
            return remote(
                pair_send.at[r], pair_recv.at[q, r], pair_ssem.at[r], pair_rsem.at[q, r],
                (sec, other),
            )

        def rs_copy(h, t):
            r = h * (chips - 1) + t
            target = ((chip + 1 + t) % chips) * 2 + core
            return remote(
                rs_send.at[r], rs_recv.at[q, r], rs_ssem.at[r], rs_rsem.at[q, r],
                (sec, target),
            )

        def pass_on(h, t):
            pair_copy(h, t).wait_recv()
            r = h * chips + t
            both = pair_mine[r] + pair_recv[q, r].astype(F32)
            rs_send[h * (chips - 1) + t] = both.astype(BF16)
            rs_copy(h, t).start()

        for h in range(parts):

            def down(t, carry, h=h):
                aim = (chip + 1 + t) % chips
                r = h * chips + t
                theirs = jnp.dot(
                    hidden[...],
                    w_down[:, cols((2 * aim + 1 - core) * parts + h)],
                    preferred_element_type=F32,
                )
                pair_send[r] = theirs.astype(BF16)
                pair_copy(h, t).start()
                pair_mine[r] = jnp.dot(
                    hidden[...],
                    w_down[:, cols((2 * aim + core) * parts + h)],
                    preferred_element_type=F32,
                )

                @pl.when(t >= 1)
                def _():
                    pass_on(h, t - 1)

                return carry

            lax.fori_loop(0, chips, down, 0)

        def z_copy(h):
            u = me * parts + h
            return remote(out_send.at[h], outs.at[q, u], z_ssem.at[h], ag_rsem.at[q, u], (after, me))

        for h in range(parts):
            pair_copy(h, chips - 1).wait_recv()
            r = h * chips + chips - 1
            total = pair_mine[r] + pair_recv[q, r].astype(F32)

            def collect(t, value, h=h):
                rs_copy(h, t).wait_recv()
                return value + rs_recv[q, h * (chips - 1) + t].astype(F32)

            total = lax.fori_loop(0, chips - 1, collect, total)
            out_send[h] = (x[:, cols(me * parts + h)] + total).astype(BF16)
            z_copy(h).start()

        def ag_copy(u, slot, device):
            return remote(
                outs.at[q, u], outs.at[q, u], ag_ssem.at[slot], ag_rsem.at[q, u], device
            )

        def absorb(u, fresh=False):
            image = inj[:, cols(u)] + 0.5 * outs[q, u].astype(F32)
            misfits[k, :, cols(u)] = image - x[:, cols(u)]

            @pl.when(k < ITERS - 1)
            def _():
                project(k, u, image, fresh)

            add_gram(k, u)

        for h in range(parts):
            u = me * parts + h
            z_copy(h).wait_recv()

            def spread(t, carry, h=h, u=u):
                target = ((chip + 1 + t) % chips) * 2 + core
                ag_copy(u, h * 2 * chips + t, (sec, target)).start()
                return carry

            lax.fori_loop(0, chips - 1, spread, 0)
            ag_copy(u, h * 2 * chips + chips - 1, (sec, other)).start()
            absorb(u, h == 0)
            u = other * parts + h
            ag_copy(u, 0, (sec, other)).wait_recv()
            absorb(u)

        def forward(i, carry):
            h, t = i // (chips - 1), i % (chips - 1)
            u = (((chip + chips - 1 - t) % chips) * 2 + core) * parts + h
            onward = ag_copy(u, h * 2 * chips + chips + t, (sec, other))
            onward.wait_recv()
            onward.start()
            absorb(u)
            return carry

        lax.fori_loop(0, parts * (chips - 1), forward, 0)

        def last(i, carry):
            h, t = i // (chips - 1), i % (chips - 1)
            u = (((chip + chips - 1 - t) % chips) * 2 + 1 - core) * parts + h
            ag_copy(u, 0, (sec, other)).wait_recv()
            absorb(u)
            return carry

        lax.fori_loop(0, parts * (chips - 1), last, 0)
        finish(k)

        for h in range(parts):

            def drain(t, carry, h=h):
                pair_copy(h, t).wait_send()
                return carry

            lax.fori_loop(0, chips, drain, 0)

            def drain_rs(t, carry, h=h):
                rs_copy(h, t).wait_send()
                return carry

            lax.fori_loop(0, chips - 1, drain_rs, 0)
            z_copy(h).wait_send()

            def drain_ag(t, carry, h=h):
                ag_copy(me * parts + h, h * 2 * chips + t, (sec, other)).wait_send()
                return carry

            lax.fori_loop(0, 2 * chips - 1, drain_ag, 0)
        return carry

    lax.fori_loop(1, ITERS, iteration, 0)
    out_ref[...] = x[pl.ds(pl.multiple_of(me * rows, rows), rows), :]


def solution(mesh):
    n_sec, n_dp = mesh.shape["section"], mesh.shape["dp"]
    chips = n_dp // 2

    def local(inject, w_gate, w_up, w_down, gain):
        rows, feats = inject.shape[1:]
        hid = w_gate.shape[2]
        tokens = rows * n_dp
        parts = 1
        block = feats // (n_dp * parts)
        rounds = ITERS - 1
        vmem = pl.BlockSpec(memory_space=pltpu.VMEM)
        hbm = pl.BlockSpec(memory_space=pl.ANY)
        dma = pltpu.SemaphoreType.DMA
        out, mixing = pl.pallas_call(
            functools.partial(kernel, n_sec, n_dp),
            out_shape=(
                jax.ShapeDtypeStruct((rows, feats), F32),
                jax.ShapeDtypeStruct((ITERS, HIST), F32),
            ),
            in_specs=[vmem, hbm, hbm, hbm, vmem],
            out_specs=(vmem, pl.BlockSpec(memory_space=pltpu.SMEM)),
            scratch_shapes=[
                pltpu.VMEM((feats, hid), BF16),
                pltpu.VMEM((feats, hid), BF16),
                pltpu.VMEM((hid, feats), BF16),
                pltpu.VMEM((2, 3, hid, block), BF16),
                pltpu.VMEM((n_dp, rows, feats), BF16),
                pltpu.VMEM((tokens, feats), F32),
                pltpu.VMEM((tokens, feats), F32),
                pltpu.VMEM((rounds, tokens, hid), F32),
                pltpu.VMEM((rounds, tokens, hid), F32),
                pltpu.VMEM((tokens, 128), F32),
                pltpu.VMEM((tokens, hid), BF16),
                pltpu.VMEM((rounds, n_dp * parts, tokens, block), BF16),
                pltpu.VMEM((HIST, tokens, feats), F32),
                pltpu.VMEM((HIST, 8, block), F32),
                pltpu.VMEM((HIST, HIST, 8, 128), F32),
                pltpu.VMEM((parts * chips, tokens, block), BF16),
                pltpu.VMEM((rounds, parts * chips, tokens, block), BF16),
                pltpu.VMEM((parts * chips, tokens, block), F32),
                pltpu.VMEM((parts * (chips - 1), tokens, block), BF16),
                pltpu.VMEM((rounds, parts * (chips - 1), tokens, block), BF16),
                pltpu.VMEM((parts, tokens, block), BF16),
                pltpu.SMEM((HIST,), F32),
                dma((3, n_dp * parts)),
                dma((n_dp,)),
                dma((n_dp,)),
                dma((parts * chips,)),
                dma((rounds, parts * chips)),
                dma((parts * chips,)),
                dma((rounds, parts * chips)),
                dma((parts,)),
                dma((2 * chips * parts,)),
                dma((rounds, n_dp * parts)),
            ],
            compiler_params=pltpu.CompilerParams(
                collective_id=0,
                has_side_effects=True,
                vmem_limit_bytes=67043328,
            ),
        )(inject[0], jnp.swapaxes(w_gate, 1, 2), jnp.swapaxes(w_up, 1, 2), w_down, gain)
        return out[None], mixing[None]

    placed = (
        P("section", "dp", None),
        P("section", None, "dp"),
        P("section", None, "dp"),
        P("section", "dp", None),
        P("section", None),
    )
    return jax.shard_map(
        local,
        mesh=mesh,
        in_specs=placed,
        out_specs=(P("section", "dp", None), P("section", None, None)),
        check_vma=False,
    )
```
